32 devices in a mesh: rep: 2 (over z, core), dp: 16 (over x, y).
Axes of the slice: x: 4, y: 4, z: 1, core: 2. Of those that a mesh axis runs over, the one named last changes fastest.
The devices are a block of a 4x4x8 slice.
Arguments:
- x: bfloat16 [32, 2048, 512], P(('rep', 'dp')), parts along dimension 0
- dy: bfloat16 [32, 2048, 512], P(('rep', 'dp')), parts along dimension 0
- w_gate: bfloat16 [2, 512, 2048], replicated
- w_up: bfloat16 [2, 512, 2048], replicated
- w_down: bfloat16 [2, 2048, 512], replicated
- m_w_gate: float32 [2, 512, 2048], replicated
- m_w_up: float32 [2, 512, 2048], replicated
- m_w_down: float32 [2, 2048, 512], replicated
- v_w_gate: float32 [2, 512, 2048], replicated
- v_w_up: float32 [2, 512, 2048], replicated
- v_w_down: float32 [2, 2048, 512], replicated
Outputs:
- output 1: bfloat16 [4, 512, 2048], P('rep'), parts along dimension 0
- output 2: bfloat16 [4, 512, 2048], P('rep'), parts along dimension 0
- output 3: bfloat16 [4, 2048, 512], P('rep'), parts along dimension 0
- output 4: float32 [4, 512, 2048], P('rep'), parts along dimension 0
- output 5: float32 [4, 512, 2048], P('rep'), parts along dimension 0
- output 6: float32 [4, 2048, 512], P('rep'), parts along dimension 0
- output 7: float32 [4, 512, 2048], P('rep'), parts along dimension 0
- output 8: float32 [4, 512, 2048], P('rep'), parts along dimension 0
- output 9: float32 [4, 2048, 512], P('rep'), parts along dimension 0
There are 2 independent parts. The reference program is written for one: setup_inputs(seed, part) draws one part's arguments, and reference() takes and returns one part's arrays. A program takes and returns all parts, laid end to end along the dimension named above; an argument that names none is the same for every part.
All inputs are finite; a program needn't handle non-finite values.
Results may differ from the reference program's by a relative error of at most 0.02.
Values are sent between devices in bfloat16 or wider.
A program may use at most 768 MiB of HBM per device.

```python
import jax
import jax.numpy as jnp
from jax import lax

SEQUENCES = 16
TOKENS = 2048
D = 512
FF = 2048
LAYERS = 2
NAMES = ("w_gate", "w_up", "w_down")
SHAPES = {"w_gate": (LAYERS, D, FF), "w_up": (LAYERS, D, FF), "w_down": (LAYERS, FF, D)}


def bump(key, n, height):
    away = (jnp.arange(n, dtype=jnp.int32) - jax.random.randint(key, (), 0, n, jnp.int32)) % n
    return jnp.where(away < n // 8, height, 1.0)


def together(key, own, strength):
    shared = jax.random.normal(key, own.shape[1:], jnp.float32)
    return (own + strength * shared) * lax.rsqrt(1 + strength * strength)


def setup_inputs(seed: int = 0, part: int = 0) -> dict:
    kx, kdy, ka, kb, kz, kf, kh, kl, *keys = jax.random.split(jax.random.key(seed), 8 + 3 * len(NAMES))
    kx, kdy, ka, kb = (jax.random.fold_in(k, part) for k in (kx, kdy, ka, kb))
    kw, km, kv = (keys[i::3] for i in range(3))
    shape = (SEQUENCES, TOKENS, D)
    much_x, much_dy = jax.random.uniform(kz, (2,), jnp.float32, 0.0, 1.0)
    loud = 2.0 ** jax.random.uniform(jax.random.fold_in(kz, 1), (), jnp.float32, -1.0, 2.0)
    layers = 2.0 ** jax.random.uniform(kl, (LAYERS, 1, 1), jnp.float32, -1.0, 1.0)
    x = together(ka, jax.random.normal(kx, shape, jnp.float32), much_x) * bump(kf, D, 4.0)
    dy = together(kb, jax.random.normal(kdy, shape, jnp.float32), much_dy)
    drawn = {"x": x.astype(jnp.bfloat16), "dy": (loud * dy * (SEQUENCES * TOKENS) ** -0.5).astype(jnp.bfloat16)}
    for key, name in zip(kw, NAMES, strict=True):
        w = jax.random.normal(key, SHAPES[name], jnp.float32) * SHAPES[name][1] ** -0.5
        drawn[name] = (w * {"w_gate": 1.0, "w_up": bump(kh, FF, 4.0), "w_down": layers}[name]).astype(jnp.bfloat16)
    for key, name in zip(km, NAMES, strict=True):
        drawn[f"m_{name}"] = 0.1 * jax.random.normal(key, SHAPES[name], jnp.float32)
    for key, name in zip(kv, NAMES, strict=True):
        drawn[f"v_{name}"] = jax.random.uniform(key, SHAPES[name], jnp.float32, 0.005, 0.015)
    return drawn


def matmul(a, w):
    return jnp.dot(a, w, preferred_element_type=jnp.float32).astype(jnp.bfloat16)


def normed(h):
    wide = h.astype(jnp.float32)
    scale = lax.rsqrt(jnp.mean(wide**2, -1, keepdims=True) + 1e-6)
    return (wide * scale).astype(jnp.bfloat16)


def layer(h, w):
    a = normed(h)
    gate = jnp.dot(a, w["w_gate"], preferred_element_type=jnp.float32)
    up = jnp.dot(a, w["w_up"], preferred_element_type=jnp.float32)
    return h + matmul((jax.nn.silu(gate) * up).astype(jnp.bfloat16), w["w_down"])


def adamw(w, m, v, g):
    m = 0.9 * m + 0.1 * g
    v = 0.95 * v + 0.05 * g * g
    step = m * lax.rsqrt(v + 1e-8) + 0.1 * w
    return (w - 0.02 * step).astype(jnp.bfloat16), m, v


def stack(weights, h):
    return lax.scan(lambda h, w: (layer(h, w), None), h, weights)[0]


def reference(x, dy, w_gate, w_up, w_down, m_w_gate, m_w_up, m_w_down, v_w_gate, v_w_up, v_w_down):
    weights = dict(zip(NAMES, (w_gate, w_up, w_down), strict=True))

    def take(so_far, sequence):
        h, by_y = sequence
        _, back = jax.vjp(lambda w: stack(w, h), weights)
        return jax.tree.map(lambda total, term: total + term.astype(jnp.float32), so_far, back(by_y)[0]), None

    none_yet = {name: jnp.zeros(w.shape, jnp.float32) for name, w in weights.items()}
    by_weights, _ = lax.scan(take, none_yet, (x, dy))
    gradients = [by_weights[name].astype(jnp.bfloat16).astype(jnp.float32) for name in NAMES]
    new = [
        adamw(w.astype(jnp.float32), m, v, g)
        for w, m, v, g in zip((w_gate, w_up, w_down), (m_w_gate, m_w_up, m_w_down), (v_w_gate, v_w_up, v_w_down), gradients, strict=True)
    ]
    return tuple(one[which] for which in range(3) for one in new)
```

```python
import functools
import math

import jax
import jax.numpy as jnp
from jax import lax
from jax.experimental import pallas as pl
from jax.experimental.pallas import tpu as pltpu
from jax.sharding import PartitionSpec as P

F32 = jnp.float32
BF16 = jnp.bfloat16
BLOCK = 512
TILE = 256
ROUNDS = 4


def dot(a, b):
    return jnp.dot(a, b, preferred_element_type=F32)


def dot_nt(a, b):
    return lax.dot_general(a, b, (((1,), (1,)), ((), ())), preferred_element_type=F32)


def normed(wide):
    return wide * lax.rsqrt(jnp.mean(wide * wide, -1, keepdims=True) + 1e-6)


def train_kernel(n, x_hbm, dy_hbm, wg_hbm, wu_hbm, wd_hbm, out_hbm,
                 h, dy, a, at, dyt, prod, dg, du, dag, dau, wg, wu, wd,
                 mine, got_a, got_b, got_c, got_d, part, stage, whole,
                 in_sem, w_sem, rs_send, rs_recv, ag_send, ag_recv, out_sem):
    layers, d, ff = wg_hbm.shape
    tokens = x_hbm.shape[1]
    blocks = ff // BLOCK
    chunks = layers * blocks
    tiles = tokens // TILE
    side = math.isqrt(n)
    chunk_rows = mine.shape[1]
    half = chunk_rows // 2
    klass = half // side
    piece = klass // side
    cols = mine.shape[2]
    hc = cols // 2

    me = lax.axis_index("dp")
    cx, cy = me // side, me % side

    def near(c, by):
        return (c + by + side) % side

    ids = {
        "x": (near(cx, 1) * side + cy, near(cx, -1) * side + cy),
        "y": (cx * side + near(cy, 1), cx * side + near(cy, -1)),
    }
    sides = ((0, cx, cy, ids["x"], ids["y"]), (1, cy, cx, ids["y"], ids["x"]))

    def rows(base, size):
        return pl.ds(pl.multiple_of(base, 16), size)

    left, right = pl.ds(0, hc), pl.ds(hc, hc)
    lanes = (left, right)

    x_copy = pltpu.make_async_copy(x_hbm.at[0], h.at[0], in_sem.at[0])
    dy_copy = pltpu.make_async_copy(dy_hbm.at[0], dy, in_sem.at[1])

    def w_copies(l, j):
        span = pl.ds(j * BLOCK, BLOCK)
        return (
            pltpu.make_async_copy(wg_hbm.at[l, :, span], wg.at[l, j], w_sem.at[0, l, j]),
            pltpu.make_async_copy(wu_hbm.at[l, :, span], wu.at[l, j], w_sem.at[1, l, j]),
            pltpu.make_async_copy(wd_hbm.at[l, span, :], wd.at[l, j], w_sem.at[2, l, j]),
        )

    x_copy.start()
    for l in range(layers):
        for j in range(blocks):
            for copy in w_copies(l, j):
                copy.start()
    dy_copy.start()

    barrier = pltpu.get_barrier_semaphore()
    for other in (*ids["x"], *ids["y"]):
        pl.semaphore_signal(barrier, inc=1, device_id={"dp": other}, device_id_type=pl.DeviceIdType.MESH)
    pl.semaphore_wait(barrier, 4)

    def rs_copy(c, hf, rnd, way, src, dst, to):
        slot = c % 2
        return pltpu.make_async_remote_copy(
            src_ref=src, dst_ref=dst, send_sem=rs_send.at[slot, hf, rnd, way], recv_sem=rs_recv.at[slot, hf, rnd, way],
            device_id={"dp": to}, device_id_type=pl.DeviceIdType.MESH)

    def rs_round(c, rnd):
        slot = c % 2
        copies = []
        for hf, f, s, fid, sid in sides:
            base = hf * half
            for way, by in ((0, 1), (1, -1)):
                if rnd == 0:
                    src = mine.at[slot, rows(base + near(f, 2) * klass, klass), lanes[way]]
                    dst, to = got_a.at[slot, hf, way], fid[way]
                elif rnd == 1:
                    src = mine.at[slot, rows(base + near(f, by) * klass, klass), :]
                    dst, to = got_b.at[slot, hf, way], fid[way]
                elif rnd == 2:
                    src = stage.at[slot, hf, 2, :, lanes[way]]
                    dst, to = got_c.at[slot, hf, way], sid[way]
                else:
                    src = stage.at[slot, hf, way]
                    dst, to = got_d.at[slot, hf, way], sid[way]
                copies.append(rs_copy(c, hf, rnd, way, src, dst, to))
        return copies

    def rs_event(c, e):
        slot = c % 2
        if e > 0:
            for copy in rs_round(c, e - 1):
                copy.wait()
        for hf, f, s, fid, sid in sides:
            base = hf * half
            if e == 1:
                for way, by in ((0, 1), (1, -1)):
                    span = rows(base + near(f, by) * klass, klass)
                    total = mine[slot, span, lanes[way]].astype(F32) + got_a[slot, hf, way].astype(F32)
                    mine[slot, span, lanes[way]] = total.astype(BF16)
            elif e == 2:
                total = mine[slot, rows(base + f * klass, klass), :].astype(F32)
                part[slot, hf] = total + got_b[slot, hf, 0].astype(F32) + got_b[slot, hf, 1].astype(F32)
                stage[slot, hf, 2] = part[slot, hf, rows(near(s, 2) * piece, piece), :].astype(BF16)
            elif e == 3:
                for way, by in ((0, 1), (1, -1)):
                    span = rows(near(s, by) * piece, piece)
                    total = part[slot, hf, span, lanes[way]] + got_c[slot, hf, way].astype(F32)
                    stage[slot, hf, way, :, lanes[way]] = total.astype(BF16)
                    stage[slot, hf, way, :, lanes[1 - way]] = part[slot, hf, span, lanes[1 - way]].astype(BF16)
            elif e == 4:
                total = part[slot, hf, rows(s * piece, piece), :]
                total = total + got_d[slot, hf, 0].astype(F32) + got_d[slot, hf, 1].astype(F32)
                whole[c, rows(base + f * klass + s * piece, piece), :] = total.astype(BF16)
        if e < ROUNDS:
            for copy in rs_round(c, e):
                copy.start()

    def ag_round(c, rnd):
        copies = []
        for hf, f, s, fid, sid in sides:
            base = hf * half
            for way, by in ((0, 1), (1, -1)):
                if rnd == 0:
                    ref = whole.at[c, rows(base + f * klass + s * piece, piece), :]
                elif rnd == 1:
                    ref = whole.at[c, rows(base + f * klass + near(s, -by) * piece, piece), lanes[way]]
                elif rnd == 2:
                    ref = whole.at[c, rows(base + f * klass, klass), :]
                else:
                    ref = whole.at[c, rows(base + near(f, -by) * klass, klass), lanes[way]]
                to = sid[way] if rnd < 2 else fid[way]
                copies.append(pltpu.make_async_remote_copy(
                    src_ref=ref, dst_ref=ref, send_sem=ag_send.at[c, hf, rnd, way], recv_sem=ag_recv.at[c, hf, rnd, way],
                    device_id={"dp": to}, device_id_type=pl.DeviceIdType.MESH))
        return copies

    def out_copy(c):
        return pltpu.make_async_copy(whole.at[c], out_hbm.at[c], out_sem.at[c])

    def ag_event(c, e):
        if e > 0:
            for copy in ag_round(c, e - 1):
                copy.wait()
        if e < ROUNDS:
            for copy in ag_round(c, e):
                copy.start()
        else:
            out_copy(c).start()

    def guarded(low, high, c, event, e):
        pl.when((c >= low) & (c < high))(lambda: event(c, e))

    def first_ticks(c):
        guarded(0, chunks, c - 2, rs_event, 3)
        guarded(0, chunks, c - 1, rs_event, 1)

    def second_ticks(c):
        guarded(0, chunks, c - 2, rs_event, 4)
        guarded(0, chunks, c - 1, rs_event, 2)
        guarded(0, chunks, c, rs_event, 0)

    x_copy.wait()
    for l in range(layers - 1):
        for j in range(blocks):
            for copy in w_copies(l, j):
                copy.wait()

        def forward(t, _):
            span = rows(t * TILE, TILE)
            wide = h[l, span, :].astype(F32)
            av = normed(wide).astype(BF16)
            acc = None
            for j in range(blocks):
                gate, up = dot(av, wg[l, j]), dot(av, wu[l, j])
                p = (gate * jax.nn.sigmoid(gate) * up).astype(BF16)
                term = dot(p, wd[l, j])
                acc = term if acc is None else acc + term
            h[l + 1, span, :] = (wide + acc.astype(BF16).astype(F32)).astype(BF16)
            return 0

        lax.fori_loop(0, tiles, forward, 0)

    for j in range(blocks):
        for copy in w_copies(layers - 1, j):
            copy.wait()
    dy_copy.wait()

    for number, l in enumerate(reversed(range(layers))):
        need = l > 0

        def enter(t, _):
            span = rows(t * TILE, TILE)
            across = pl.ds(pl.multiple_of(t * TILE, 128), TILE)
            av = normed(h[l, span, :].astype(F32))
            a[span, :] = av.astype(BF16)
            at[:, across] = av.T.astype(BF16)
            dyt[:, across] = dy[span, :].astype(F32).T.astype(BF16)
            if need:
                dag[span, :] = jnp.zeros((TILE, d), F32)
                dau[span, :] = jnp.zeros((TILE, d), F32)
            return 0

        lax.fori_loop(0, tiles, enter, 0)

        def block(j, _):
            c = number * blocks + j
            slot = c % 2

            def tile(t, _):
                span = rows(t * TILE, TILE)
                av, dyv = a[span, :], dy[span, :]
                gate, up = dot(av, wg[l, j]), dot(av, wu[l, j])
                dp = dot_nt(dyv, wd[l, j]).astype(BF16).astype(F32)
                sig = jax.nn.sigmoid(gate)
                act = gate * sig
                prod[span, :] = (act * up).astype(BF16)
                dgv = (dp * up * (sig + act * (1.0 - sig))).astype(BF16)
                duv = (dp * act).astype(BF16)
                dg[span, :] = dgv
                du[span, :] = duv
                if need:
                    dag[span, :] += dot_nt(dgv, wg[l, j])
                    dau[span, :] += dot_nt(duv, wu[l, j])
                return 0

            cut = tiles * 3 // 4 if need else tiles
            lax.fori_loop(0, cut, tile, 0)
            first_ticks(c)
            if cut < tiles:
                lax.fori_loop(cut, tiles, tile, 0)

            def grads(q, _):
                span = rows(q * 256, 256)
                mine[slot, span, :] = dot(at[span, :], dg[...]).astype(BF16)
                mine[slot, rows(d + q * 256, 256), :] = dot(at[span, :], du[...]).astype(BF16)
                across = pl.ds(pl.multiple_of(q * 256, 128), 256)
                mine[slot, 2 * d : 2 * d + BLOCK, across] = dot(dyt[span, :], prod[...]).T.astype(BF16)
                return 0

            lax.fori_loop(0, d // 256, grads, 0)
            second_ticks(c)
            return 0

        lax.fori_loop(0, blocks, block, 0)

        if need:

            def leave(t, _):
                span = rows(t * TILE, TILE)
                da = (dag[span, :].astype(BF16).astype(F32) + dau[span, :].astype(BF16).astype(F32)).astype(BF16).astype(F32)
                wide = h[l, span, :].astype(F32)
                scale = lax.rsqrt(jnp.mean(wide * wide, -1, keepdims=True) + 1e-6)
                by_scale = jnp.sum(da * wide, -1, keepdims=True)
                by_wide = da * scale - wide * (by_scale * scale * scale * scale * (1.0 / d))
                dy[span, :] = (dy[span, :].astype(F32) + by_wide.astype(BF16).astype(F32)).astype(BF16)
                return 0

            lax.fori_loop(0, tiles, leave, 0)

    def drain(k, _):
        for e in (4, 3, 2, 1):
            guarded(0, chunks, k - e, ag_event, e)
        pl.when(k == 0)(lambda: first_ticks(chunks))
        pl.when(k == 1)(lambda: second_ticks(chunks))
        pl.when(k == 2)(lambda: first_ticks(chunks + 1))
        pl.when(k == 3)(lambda: second_ticks(chunks + 1))
        guarded(0, chunks, k, ag_event, 0)
        return 0

    lax.fori_loop(0, chunks + ROUNDS, drain, 0)
    for c in range(chunks):
        out_copy(c).wait()


def summed_gradients(n, x, dy, wg, wu, wd):
    layers, d, ff = wg.shape
    tokens = x.shape[1]
    blocks = ff // BLOCK
    chunks = layers * blocks
    side = math.isqrt(n)
    chunk_rows = 2 * d + BLOCK
    klass = chunk_rows // 2 // side
    piece = klass // side
    hbm = pl.BlockSpec(memory_space=pl.ANY)
    dma = pltpu.SemaphoreType.DMA
    return pl.pallas_call(
        functools.partial(train_kernel, n),
        out_shape=jax.ShapeDtypeStruct((chunks, chunk_rows, d), BF16),
        in_specs=[hbm] * 5,
        out_specs=hbm,
        scratch_shapes=[
            pltpu.VMEM((layers, tokens, d), BF16),
            pltpu.VMEM((tokens, d), BF16),
            pltpu.VMEM((tokens, d), BF16),
            pltpu.VMEM((d, tokens), BF16),
            pltpu.VMEM((d, tokens), BF16),
            pltpu.VMEM((tokens, BLOCK), BF16),
            pltpu.VMEM((tokens, BLOCK), BF16),
            pltpu.VMEM((tokens, BLOCK), BF16),
            pltpu.VMEM((tokens, d), F32),
            pltpu.VMEM((tokens, d), F32),
            pltpu.VMEM((layers, blocks, d, BLOCK), BF16),
            pltpu.VMEM((layers, blocks, d, BLOCK), BF16),
            pltpu.VMEM((layers, blocks, BLOCK, d), BF16),
            pltpu.VMEM((2, chunk_rows, d), BF16),
            pltpu.VMEM((2, 2, 2, klass, d // 2), BF16),
            pltpu.VMEM((2, 2, 2, klass, d), BF16),
            pltpu.VMEM((2, 2, 2, piece, d // 2), BF16),
            pltpu.VMEM((2, 2, 2, piece, d), BF16),
            pltpu.VMEM((2, 2, klass, d), F32),
            pltpu.VMEM((2, 2, 3, piece, d), BF16),
            pltpu.VMEM((chunks, chunk_rows, d), BF16),
            dma((2,)),
            dma((3, layers, blocks)),
            dma((2, 2, ROUNDS, 2)),
            dma((2, 2, ROUNDS, 2)),
            dma((chunks, 2, ROUNDS, 2)),
            dma((chunks, 2, ROUNDS, 2)),
            dma((chunks,)),
        ],
        compiler_params=pltpu.CompilerParams(collective_id=0, has_side_effects=True, vmem_limit_bytes=67043328),
        name="train",
    )(x, dy, wg, wu, wd)


def adamw_kernel(g, *refs):
    ins, outs = refs[:9], refs[9:]
    for i in range(3):
        w, m, v = (ins[i + 3 * k] for k in range(3))
        gv = g[0, i].astype(F32)
        mv = 0.9 * m[0] + 0.1 * gv
        vv = 0.95 * v[0] + 0.05 * gv * gv
        wv = w[0].astype(F32)
        step = mv * lax.rsqrt(vv + 1e-8) + 0.1 * wv
        outs[i][0] = (wv - 0.02 * step).astype(BF16)
        outs[i + 3][0] = mv
        outs[i + 6][0] = vv


def adamw(g, arrays):
    layers, d, ff = arrays[0].shape
    blocks = ff // BLOCK
    cut = 2
    size = d // cut
    g = g.reshape(layers * blocks, 3, d, BLOCK)
    wide = pl.BlockSpec((1, size, BLOCK), lambda c, r: (layers - 1 - c // blocks, r, c % blocks))
    tall = pl.BlockSpec((1, size, d), lambda c, r: (layers - 1 - c // blocks, (c % blocks) * cut + r, 0))
    specs = [wide, wide, tall] * 3
    return pl.pallas_call(
        adamw_kernel,
        grid=(layers * blocks, cut),
        out_shape=[jax.ShapeDtypeStruct(v.shape, v.dtype) for v in arrays],
        in_specs=[pl.BlockSpec((1, 3, size, BLOCK), lambda c, r: (c, 0, r, 0)), *specs],
        out_specs=specs,
        compiler_params=pltpu.CompilerParams(vmem_limit_bytes=60 * 2**20),
        name="adamw",
    )(g, *arrays)


def solution(mesh):
    n = mesh.shape["dp"]

    def step(x, dy, *arrays):
        g = summed_gradients(n, x, dy, *arrays[:3])
        return tuple(adamw(g, arrays))

    return jax.shard_map(
        step,
        mesh=mesh,
        in_specs=(P(("rep", "dp"), None, None),) * 2 + (P(None, None, None),) * 9,
        out_specs=(P("rep", None, None),) * 9,
        check_vma=False,
    )
```

```python
import functools
import math

import jax
import jax.numpy as jnp
from jax import lax
from jax.experimental import pallas as pl
from jax.experimental.pallas import tpu as pltpu
from jax.sharding import PartitionSpec as P

F32 = jnp.float32
BF16 = jnp.bfloat16
BLOCK = 512
TILE = 512
ROUNDS = 4
SCATTER_AT = (0, 1, 3, 4, 5)
GATHER_AT = (5, 6, 9, 12, 15)


def dot(a, b):
    return jnp.dot(a, b, preferred_element_type=F32)


def dot_nt(a, b):
    return lax.dot_general(a, b, (((1,), (1,)), ((), ())), preferred_element_type=F32)


def sigmoid(x):
    return 0.5 * jnp.tanh(0.5 * x) + 0.5


def normed(wide):
    return wide * lax.rsqrt(jnp.mean(wide * wide, -1, keepdims=True) + 1e-6)


def train_kernel(n, x_hbm, dy_hbm, wg_hbm, wu_hbm, wd_hbm, out_hbm,
                 h, dy, a, at, dyt, prod, dg, du, dag, dau, weights,
                 mine, got_a, got_b, got_c, got_d, part, stage, whole,
                 in_sem, w_sem, rs_send, rs_recv, ag_send, ag_recv, out_sem):
    layers, d, ff = wg_hbm.shape
    tokens = x_hbm.shape[1]
    blocks = ff // BLOCK
    chunks = layers * blocks
    tiles = tokens // TILE
    side = math.isqrt(n)
    chunk_rows = mine.shape[1]
    half = chunk_rows // 2
    klass = half // side
    piece = klass // side
    cols = mine.shape[2]
    hc = cols // 2

    me = lax.axis_index("dp")
    cx, cy = me // side, me % side

    def near(c, by):
        return (c + by + side) % side

    ids = {
        "x": (near(cx, 1) * side + cy, near(cx, -1) * side + cy),
        "y": (cx * side + near(cy, 1), cx * side + near(cy, -1)),
    }
    sides = ((0, cx, cy, ids["x"], ids["y"]), (1, cy, cx, ids["y"], ids["x"]))

    def rows(base, size):
        return pl.ds(pl.multiple_of(base, 16), size)

    left, right = pl.ds(0, hc), pl.ds(hc, hc)
    lanes = (left, right)

    w_rows = (pl.ds(0, d), pl.ds(d, d), pl.ds(2 * d, BLOCK))

    def w_place(l, j):
        return (whole, chunks - blocks + j) if l == layers - 1 else (weights, l * blocks + j)

    def w_read(l, j, k):
        ref, i = w_place(l, j)
        return ref[i, w_rows[k], :]

    x_copy = pltpu.make_async_copy(x_hbm.at[0], h.at[0], in_sem.at[0])
    dy_copy = pltpu.make_async_copy(dy_hbm.at[0], dy, in_sem.at[1])

    def w_copies(l, j):
        span = pl.ds(j * BLOCK, BLOCK)
        ref, i = w_place(l, j)
        sources = (wg_hbm.at[l, :, span], wu_hbm.at[l, :, span], wd_hbm.at[l, span, :])
        return [pltpu.make_async_copy(src, ref.at[i, w_rows[k], :], w_sem.at[k, l, j]) for k, src in enumerate(sources)]

    x_copy.start()
    for l in range(layers):
        for j in range(blocks):
            for copy in w_copies(l, j):
                copy.start()
    dy_copy.start()

    barrier = pltpu.get_barrier_semaphore()
    for other in (*ids["x"], *ids["y"]):
        pl.semaphore_signal(barrier, inc=1, device_id={"dp": other}, device_id_type=pl.DeviceIdType.MESH)
    pl.semaphore_wait(barrier, 4)

    def rs_copy(c, hf, rnd, way, src, dst, to):
        slot = c % 2
        return pltpu.make_async_remote_copy(
            src_ref=src, dst_ref=dst, send_sem=rs_send.at[slot, hf, rnd, way], recv_sem=rs_recv.at[slot, hf, rnd, way],
            device_id={"dp": to}, device_id_type=pl.DeviceIdType.MESH)

    def rs_round(c, rnd):
        slot = c % 2
        copies = []
        for hf, f, s, fid, sid in sides:
            base = hf * half
            for way, by in ((0, 1), (1, -1)):
                if rnd == 0:
                    src = mine.at[slot, rows(base + near(f, 2) * klass, klass), lanes[way]]
                    dst, to = got_a.at[slot, hf, way], fid[way]
                elif rnd == 1:
                    src = mine.at[slot, rows(base + near(f, by) * klass, klass), :]
                    dst, to = got_b.at[slot, hf, way], fid[way]
                elif rnd == 2:
                    src = stage.at[slot, hf, 2, :, lanes[way]]
                    dst, to = got_c.at[slot, hf, way], sid[way]
                else:
                    src = stage.at[slot, hf, way]
                    dst, to = got_d.at[slot, hf, way], sid[way]
                copies.append(rs_copy(c, hf, rnd, way, src, dst, to))
        return copies

    def rs_event(c, e):
        slot = c % 2
        if e > 0:
            for copy in rs_round(c, e - 1):
                copy.wait()
        for hf, f, s, fid, sid in sides:
            base = hf * half
            if e == 1:
                for way, by in ((0, 1), (1, -1)):
                    span = rows(base + near(f, by) * klass, klass)
                    total = mine[slot, span, lanes[way]].astype(F32) + got_a[slot, hf, way].astype(F32)
                    mine[slot, span, lanes[way]] = total.astype(BF16)
            elif e == 2:
                total = mine[slot, rows(base + f * klass, klass), :].astype(F32)
                part[slot, hf] = total + got_b[slot, hf, 0].astype(F32) + got_b[slot, hf, 1].astype(F32)
                stage[slot, hf, 2] = part[slot, hf, rows(near(s, 2) * piece, piece), :].astype(BF16)
            elif e == 3:
                for way, by in ((0, 1), (1, -1)):
                    span = rows(near(s, by) * piece, piece)
                    total = part[slot, hf, span, lanes[way]] + got_c[slot, hf, way].astype(F32)
                    stage[slot, hf, way, :, lanes[way]] = total.astype(BF16)
                    stage[slot, hf, way, :, lanes[1 - way]] = part[slot, hf, span, lanes[1 - way]].astype(BF16)
            elif e == 4:
                total = part[slot, hf, rows(s * piece, piece), :]
                total = total + got_d[slot, hf, 0].astype(F32) + got_d[slot, hf, 1].astype(F32)
                whole[c, rows(base + f * klass + s * piece, piece), :] = total.astype(BF16)
        if e < ROUNDS:
            for copy in rs_round(c, e):
                copy.start()

    def ag_round(c, rnd):
        copies = []
        for hf, f, s, fid, sid in sides:
            base = hf * half
            for way, by in ((0, 1), (1, -1)):
                if rnd == 0:
                    ref = whole.at[c, rows(base + f * klass + s * piece, piece), :]
                elif rnd == 1:
                    ref = whole.at[c, rows(base + f * klass + near(s, -by) * piece, piece), lanes[way]]
                elif rnd == 2:
                    ref = whole.at[c, rows(base + f * klass, klass), :]
                else:
                    ref = whole.at[c, rows(base + near(f, -by) * klass, klass), lanes[way]]
                to = sid[way] if rnd < 2 else fid[way]
                copies.append(pltpu.make_async_remote_copy(
                    src_ref=ref, dst_ref=ref, send_sem=ag_send.at[c, hf, rnd, way], recv_sem=ag_recv.at[c, hf, rnd, way],
                    device_id={"dp": to}, device_id_type=pl.DeviceIdType.MESH))
        return copies

    def out_copy(c):
        return pltpu.make_async_copy(whole.at[c], out_hbm.at[c], out_sem.at[c])

    def ag_event(c, e):
        if e > 0:
            for copy in ag_round(c, e - 1):
                copy.wait()
        if e < ROUNDS:
            for copy in ag_round(c, e):
                copy.start()
        else:
            out_copy(c).start()

    def tick(b, odd):
        due = [(at, 0, e) for e, at in enumerate(SCATTER_AT)] + [(at, 1, e) for e, at in enumerate(GATHER_AT)]
        for at, gather, e in sorted(due, key=lambda one: (-((one[0] + 1) // 2), one[1], one[2])):
            if (at + 1) % 2 == odd:
                c = b - (at + 1) // 2
                pl.when((c >= 0) & (c < chunks))(functools.partial(ag_event if gather else rs_event, c, e))

    x_copy.wait()
    for l in range(layers - 1):
        for j in range(blocks):
            for copy in w_copies(l, j):
                copy.wait()

        def forward(t, _):
            span = rows(t * TILE, TILE)
            wide = h[l, span, :].astype(F32)
            av = normed(wide).astype(BF16)
            acc = None
            for j in range(blocks):
                gate, up = dot(av, w_read(l, j, 0)), dot(av, w_read(l, j, 1))
                p = (gate * sigmoid(gate) * up).astype(BF16)
                term = dot(p, w_read(l, j, 2))
                acc = term if acc is None else acc + term
            h[l + 1, span, :] = (wide + acc.astype(BF16).astype(F32)).astype(BF16)
            return 0

        lax.fori_loop(0, tiles, forward, 0)

    for j in range(blocks):
        for copy in w_copies(layers - 1, j):
            copy.wait()
    dy_copy.wait()

    for number, l in enumerate(reversed(range(layers))):
        need = l > 0

        def enter(t, _):
            span = rows(t * TILE, TILE)
            across = pl.ds(pl.multiple_of(t * TILE, 128), TILE)
            av = normed(h[l, span, :].astype(F32))
            a[span, :] = av.astype(BF16)
            at[:, across] = av.T.astype(BF16)
            dyt[:, across] = dy[span, :].astype(F32).T.astype(BF16)
            if need:
                dag[span, :] = jnp.zeros((TILE, d), F32)
                dau[span, :] = jnp.zeros((TILE, d), F32)
            return 0

        lax.fori_loop(0, tiles, enter, 0)

        def block(j, _):
            c = number * blocks + j
            slot = c % 2

            def tile(t, _):
                span = rows(t * TILE, TILE)
                av, dyv = a[span, :], dy[span, :]
                gate, up = dot(av, w_read(l, j, 0)), dot(av, w_read(l, j, 1))
                dp = dot_nt(dyv, w_read(l, j, 2)).astype(BF16).astype(F32)
                sig = sigmoid(gate)
                act = gate * sig
                prod[span, :] = (act * up).astype(BF16)
                dgv = (dp * up * (sig + act * (1.0 - sig))).astype(BF16)
                duv = (dp * act).astype(BF16)
                dg[span, :] = dgv
                du[span, :] = duv
                if need:
                    dag[span, :] += dot_nt(dgv, w_read(l, j, 0))
                    dau[span, :] += dot_nt(duv, w_read(l, j, 1))
                return 0

            cut = tiles * 3 // 4 if need else tiles
            lax.fori_loop(0, cut, tile, 0)
            tick(c, 0)
            if cut < tiles:
                lax.fori_loop(cut, tiles, tile, 0)

            def grads(q, _):
                span = rows(q * 256, 256)
                mine[slot, span, :] = dot(at[span, :], dg[...]).astype(BF16)
                mine[slot, rows(d + q * 256, 256), :] = dot(at[span, :], du[...]).astype(BF16)
                across = pl.ds(pl.multiple_of(q * 256, 128), 256)
                mine[slot, 2 * d : 2 * d + BLOCK, across] = dot(dyt[span, :], prod[...]).T.astype(BF16)
                return 0

            lax.fori_loop(0, d // 256, grads, 0)
            tick(c, 1)
            return 0

        lax.fori_loop(0, blocks, block, 0)

        if need:

            def leave(t, _):
                span = rows(t * TILE, TILE)
                da = (dag[span, :].astype(BF16).astype(F32) + dau[span, :].astype(BF16).astype(F32)).astype(BF16).astype(F32)
                wide = h[l, span, :].astype(F32)
                scale = lax.rsqrt(jnp.mean(wide * wide, -1, keepdims=True) + 1e-6)
                by_scale = jnp.sum(da * wide, -1, keepdims=True)
                by_wide = da * scale - wide * (by_scale * scale * scale * scale * (1.0 / d))
                dy[span, :] = (dy[span, :].astype(F32) + by_wide.astype(BF16).astype(F32)).astype(BF16)
                return 0

            lax.fori_loop(0, tiles, leave, 0)

    def drain(b, _):
        tick(b, 0)
        tick(b, 1)
        return 0

    lax.fori_loop(chunks, chunks + (GATHER_AT[-1] + 1) // 2, drain, 0)
    for c in range(chunks):
        out_copy(c).wait()


def summed_gradients(n, x, dy, wg, wu, wd):
    layers, d, ff = wg.shape
    tokens = x.shape[1]
    blocks = ff // BLOCK
    chunks = layers * blocks
    side = math.isqrt(n)
    chunk_rows = 2 * d + BLOCK
    klass = chunk_rows // 2 // side
    piece = klass // side
    hbm = pl.BlockSpec(memory_space=pl.ANY)
    dma = pltpu.SemaphoreType.DMA
    return pl.pallas_call(
        functools.partial(train_kernel, n),
        out_shape=jax.ShapeDtypeStruct((chunks, chunk_rows, d), BF16),
        in_specs=[hbm] * 5,
        out_specs=hbm,
        scratch_shapes=[
            pltpu.VMEM((layers, tokens, d), BF16),
            pltpu.VMEM((tokens, d), BF16),
            pltpu.VMEM((tokens, d), BF16),
            pltpu.VMEM((d, tokens), BF16),
            pltpu.VMEM((d, tokens), BF16),
            pltpu.VMEM((tokens, BLOCK), BF16),
            pltpu.VMEM((tokens, BLOCK), BF16),
            pltpu.VMEM((tokens, BLOCK), BF16),
            pltpu.VMEM((tokens, d), F32),
            pltpu.VMEM((tokens, d), F32),
            pltpu.VMEM(((layers - 1) * blocks, chunk_rows, d), BF16),
            pltpu.VMEM((2, chunk_rows, d), BF16),
            pltpu.VMEM((2, 2, 2, klass, d // 2), BF16),
            pltpu.VMEM((2, 2, 2, klass, d), BF16),
            pltpu.VMEM((2, 2, 2, piece, d // 2), BF16),
            pltpu.VMEM((2, 2, 2, piece, d), BF16),
            pltpu.VMEM((2, 2, klass, d), F32),
            pltpu.VMEM((2, 2, 3, piece, d), BF16),
            pltpu.VMEM((chunks, chunk_rows, d), BF16),
            dma((2,)),
            dma((3, layers, blocks)),
            dma((2, 2, ROUNDS, 2)),
            dma((2, 2, ROUNDS, 2)),
            dma((chunks, 2, ROUNDS, 2)),
            dma((chunks, 2, ROUNDS, 2)),
            dma((chunks,)),
        ],
        compiler_params=pltpu.CompilerParams(collective_id=0, has_side_effects=True, vmem_limit_bytes=67043328),
        name="train",
    )(x, dy, wg, wu, wd)


def adamw_kernel(g, *refs):
    ins, outs = refs[:9], refs[9:]
    for i in range(3):
        w, m, v = (ins[i + 3 * k] for k in range(3))
        gv = g[0, i].astype(F32)
        mv = 0.9 * m[0] + 0.1 * gv
        vv = 0.95 * v[0] + 0.05 * gv * gv
        wv = w[0].astype(F32)
        step = mv * lax.rsqrt(vv + 1e-8) + 0.1 * wv
        outs[i][0] = (wv - 0.02 * step).astype(BF16)
        outs[i + 3][0] = mv
        outs[i + 6][0] = vv


def adamw(g, arrays):
    layers, d, ff = arrays[0].shape
    blocks = ff // BLOCK
    cut = 1
    size = d // cut
    g = g.reshape(layers * blocks, 3, d, BLOCK)
    wide = pl.BlockSpec((1, size, BLOCK), lambda c, r: (layers - 1 - c // blocks, r, c % blocks))
    tall = pl.BlockSpec((1, size, d), lambda c, r: (layers - 1 - c // blocks, (c % blocks) * cut + r, 0))
    specs = [wide, wide, tall] * 3
    return pl.pallas_call(
        adamw_kernel,
        grid=(layers * blocks, cut),
        out_shape=[jax.ShapeDtypeStruct(v.shape, v.dtype) for v in arrays],
        in_specs=[pl.BlockSpec((1, 3, size, BLOCK), lambda c, r: (c, 0, r, 0)), *specs],
        out_specs=specs,
        compiler_params=pltpu.CompilerParams(vmem_limit_bytes=60 * 2**20),
        name="adamw",
    )(g, *arrays)


def solution(mesh):
    n = mesh.shape["dp"]

    def step(x, dy, *arrays):
        g = summed_gradients(n, x, dy, *arrays[:3])
        return tuple(adamw(g, arrays))

    return jax.shard_map(
        step,
        mesh=mesh,
        in_specs=(P(("rep", "dp"), None, None),) * 2 + (P(None, None, None),) * 9,
        out_specs=(P("rep", None, None),) * 9,
        check_vma=False,
    )
```

```python
import functools
import math

import jax
import jax.numpy as jnp
from jax import lax
from jax.experimental import pallas as pl
from jax.experimental.pallas import tpu as pltpu
from jax.sharding import PartitionSpec as P

F32 = jnp.float32
BF16 = jnp.bfloat16
BLOCK = 512
TILE = 512
ROUNDS = 4
AHEAD = 16
SCATTER_AT = (0, 1, 3, 5, 7)
GATHER_AT = (7, 8, 10, 13, 17)


def dot(a, b):
    return jnp.dot(a, b, preferred_element_type=F32)


def dot_nt(a, b):
    return lax.dot_general(a, b, (((1,), (1,)), ((), ())), preferred_element_type=F32)


def sigmoid(x):
    return 0.5 * jnp.tanh(0.5 * x) + 0.5


def normed(wide):
    return wide * lax.rsqrt(jnp.mean(wide * wide, -1, keepdims=True) + 1e-6)


def train_kernel(n, x_hbm, dy_hbm, wg_hbm, wu_hbm, wd_hbm, out_hbm,
                 h, dy, a, at, dyt, prod, dg, du, weights,
                 mine, got_a, got_b, got_c, got_d, part, stage, whole,
                 in_sem, w_sem, rs_send, rs_recv, ag_send, ag_recv, out_sem):
    layers, d, ff = wg_hbm.shape
    tokens = x_hbm.shape[1]
    blocks = ff // BLOCK
    chunks = layers * blocks
    tiles = tokens // TILE
    period = blocks + tiles // 2
    side = math.isqrt(n)
    chunk_rows = mine.shape[1]
    half = chunk_rows // 2
    klass = half // side
    piece = klass // side
    cols = mine.shape[2]
    hc = cols // 2

    me = lax.axis_index("dp")
    cx, cy = me // side, me % side

    def near(c, by):
        return (c + by + side) % side

    ids = {
        "x": (near(cx, 1) * side + cy, near(cx, -1) * side + cy),
        "y": (cx * side + near(cy, 1), cx * side + near(cy, -1)),
    }
    sides = ((0, cx, cy, ids["x"], ids["y"]), (1, cy, cx, ids["y"], ids["x"]))

    def rows(base, size):
        return pl.ds(pl.multiple_of(base, 16), size)

    left, right = pl.ds(0, hc), pl.ds(hc, hc)
    lanes = (left, right)

    w_rows = (pl.ds(0, d), pl.ds(d, d), pl.ds(2 * d, BLOCK))

    def w_place(l, j):
        return (whole, chunks - blocks + j) if l == layers - 1 else (weights, l * blocks + j)

    def w_read(l, j, k):
        ref, i = w_place(l, j)
        return ref[i, w_rows[k], :]

    x_copy = pltpu.make_async_copy(x_hbm.at[0], h.at[0], in_sem.at[0])
    dy_copy = pltpu.make_async_copy(dy_hbm.at[0], dy, in_sem.at[1])

    def w_copies(l, j):
        span = pl.ds(j * BLOCK, BLOCK)
        ref, i = w_place(l, j)
        sources = (wg_hbm.at[l, :, span], wu_hbm.at[l, :, span], wd_hbm.at[l, span, :])
        return [pltpu.make_async_copy(src, ref.at[i, w_rows[k], :], w_sem.at[k, l, j]) for k, src in enumerate(sources)]

    x_copy.start()
    for l in range(layers):
        for j in range(blocks):
            for copy in w_copies(l, j):
                copy.start()
    dy_copy.start()

    barrier = pltpu.get_barrier_semaphore()
    for other in (*ids["x"], *ids["y"]):
        pl.semaphore_signal(barrier, inc=1, device_id={"dp": other}, device_id_type=pl.DeviceIdType.MESH)
    pl.semaphore_wait(barrier, 4)

    def rs_copy(c, hf, rnd, way, src, dst, to):
        slot = c % 2
        return pltpu.make_async_remote_copy(
            src_ref=src, dst_ref=dst, send_sem=rs_send.at[slot, hf, rnd, way], recv_sem=rs_recv.at[slot, hf, rnd, way],
            device_id={"dp": to}, device_id_type=pl.DeviceIdType.MESH)

    def rs_round(c, rnd):
        slot = c % 2
        copies = []
        for hf, f, s, fid, sid in sides:
            base = hf * half
            for way, by in ((0, 1), (1, -1)):
                if rnd == 0:
                    src = mine.at[slot, rows(base + near(f, 2) * klass, klass), lanes[way]]
                    dst, to = got_a.at[slot, hf, way], fid[way]
                elif rnd == 1:
                    src = mine.at[slot, rows(base + near(f, by) * klass, klass), :]
                    dst, to = got_b.at[slot, hf, way], fid[way]
                elif rnd == 2:
                    src = stage.at[slot, hf, 2, :, lanes[way]]
                    dst, to = got_c.at[slot, hf, way], sid[way]
                else:
                    src = stage.at[slot, hf, way]
                    dst, to = got_d.at[slot, hf, way], sid[way]
                copies.append(rs_copy(c, hf, rnd, way, src, dst, to))
        return copies

    def rs_event(c, e):
        slot = c % 2
        if e > 0:
            for copy in rs_round(c, e - 1):
                copy.wait()
        for hf, f, s, fid, sid in sides:
            base = hf * half
            if e == 1:
                for way, by in ((0, 1), (1, -1)):
                    span = rows(base + near(f, by) * klass, klass)
                    total = mine[slot, span, lanes[way]].astype(F32) + got_a[slot, hf, way].astype(F32)
                    mine[slot, span, lanes[way]] = total.astype(BF16)
            elif e == 2:
                total = mine[slot, rows(base + f * klass, klass), :].astype(F32)
                part[slot, hf] = total + got_b[slot, hf, 0].astype(F32) + got_b[slot, hf, 1].astype(F32)
                stage[slot, hf, 2] = part[slot, hf, rows(near(s, 2) * piece, piece), :].astype(BF16)
            elif e == 3:
                for way, by in ((0, 1), (1, -1)):
                    span = rows(near(s, by) * piece, piece)
                    total = part[slot, hf, span, lanes[way]] + got_c[slot, hf, way].astype(F32)
                    stage[slot, hf, way, :, lanes[way]] = total.astype(BF16)
                    stage[slot, hf, way, :, lanes[1 - way]] = part[slot, hf, span, lanes[1 - way]].astype(BF16)
            elif e == 4:
                total = part[slot, hf, rows(s * piece, piece), :]
                total = total + got_d[slot, hf, 0].astype(F32) + got_d[slot, hf, 1].astype(F32)
                whole[c, rows(base + f * klass + s * piece, piece), :] = total.astype(BF16)
        if e < ROUNDS:
            for copy in rs_round(c, e):
                copy.start()

    def ag_round(c, rnd):
        copies = []
        for hf, f, s, fid, sid in sides:
            base = hf * half
            for way, by in ((0, 1), (1, -1)):
                if rnd == 0:
                    ref = whole.at[c, rows(base + f * klass + s * piece, piece), :]
                elif rnd == 1:
                    ref = whole.at[c, rows(base + f * klass + near(s, -by) * piece, piece), lanes[way]]
                elif rnd == 2:
                    ref = whole.at[c, rows(base + f * klass, klass), :]
                else:
                    ref = whole.at[c, rows(base + near(f, -by) * klass, klass), lanes[way]]
                to = sid[way] if rnd < 2 else fid[way]
                copies.append(pltpu.make_async_remote_copy(
                    src_ref=ref, dst_ref=ref, send_sem=ag_send.at[c, hf, rnd, way], recv_sem=ag_recv.at[c, hf, rnd, way],
                    device_id={"dp": to}, device_id_type=pl.DeviceIdType.MESH))
        return copies

    def out_copy(c):
        return pltpu.make_async_copy(whole.at[c], out_hbm.at[c], out_sem.at[c])

    def ag_event(c, e):
        if e > 0:
            for copy in ag_round(c, e - 1):
                copy.wait()
        if e < ROUNDS:
            for copy in ag_round(c, e):
                copy.start()
        else:
            out_copy(c).start()

    def tick(b, odd):
        due = [(at, 0, e) for e, at in enumerate(SCATTER_AT)] + [(at, 1, e) for e, at in enumerate(GATHER_AT)]
        for at, gather, e in sorted(due, key=lambda one: (-((one[0] + 1) // 2), one[1], one[2])):
            if (at + 1) % 2 == odd:
                back = b - (at + 1) // 2 + period * AHEAD
                number, j = lax.div(back, period) - AHEAD, lax.rem(back, period)
                event = functools.partial(ag_event if gather else rs_event, number * blocks + j, e)
                pl.when((number >= 0) & (number < layers) & (j < blocks))(event)

    x_copy.wait()
    for l in range(layers - 1):
        def arrived(l, j):
            for copy in w_copies(l, j):
                copy.wait()

        def forward(t, _):
            span = rows(t * TILE, TILE)
            wide = h[l, span, :].astype(F32)
            av = normed(wide).astype(BF16)
            acc = None
            for j in range(blocks):
                pl.when(t == 0)(functools.partial(arrived, l, j))
                gate, up = dot(av, w_read(l, j, 0)), dot(av, w_read(l, j, 1))
                p = (gate * sigmoid(gate) * up).astype(BF16)
                term = dot(p, w_read(l, j, 2))
                acc = term if acc is None else acc + term
            h[l + 1, span, :] = (wide + acc.astype(BF16).astype(F32)).astype(BF16)
            return 0

        lax.fori_loop(0, tiles, forward, 0)

    for j in range(blocks):
        for copy in w_copies(layers - 1, j):
            copy.wait()
    dy_copy.wait()

    def enter(l, t):
        span = rows(t * TILE, TILE)
        across = pl.ds(pl.multiple_of(t * TILE, 128), TILE)
        av = normed(h[l, span, :].astype(F32)).astype(BF16)
        a[span, :] = av
        at[:, across] = av.T
        dyt[:, across] = dy[span, :].T

    def leave(l, t):
        span = rows(t * TILE, TILE)

        def back(grads, k):
            total = None
            for j in range(blocks):
                term = dot_nt(grads[j, span, :], w_read(l, j, k))
                total = term if total is None else total + term
            return total.astype(BF16).astype(F32)

        da = (back(dg, 0) + back(du, 1)).astype(BF16).astype(F32)
        wide = h[l, span, :].astype(F32)
        scale = lax.rsqrt(jnp.mean(wide * wide, -1, keepdims=True) + 1e-6)
        by_scale = jnp.sum(da * wide, -1, keepdims=True)
        by_wide = da * scale - wide * (by_scale * scale * scale * scale * (1.0 / d))
        dy[span, :] = (dy[span, :].astype(F32) + by_wide.astype(BF16).astype(F32)).astype(BF16)

    def first(t, _):
        enter(layers - 1, t)
        return 0

    lax.fori_loop(0, tiles, first, 0)
    for number, l in enumerate(reversed(range(layers))):

        def block(j, _):
            c = number * blocks + j
            slot = c % 2

            def tile(t, _):
                span = rows(t * TILE, TILE)
                av, dyv = a[span, :], dy[span, :]
                gate, up = dot(av, w_read(l, j, 0)), dot(av, w_read(l, j, 1))
                dp = dot_nt(dyv, w_read(l, j, 2)).astype(BF16).astype(F32)
                sig = sigmoid(gate)
                act = gate * sig
                prod[span, :] = (act * up).astype(BF16)
                dgv = (dp * up * (sig + act * (1.0 - sig))).astype(BF16)
                duv = (dp * act).astype(BF16)
                dg[j, span, :] = dgv
                du[j, span, :] = duv
                return 0

            lax.fori_loop(0, tiles, tile, 0)
            tick(number * period + j, 0)
            mine[slot, 0:d, :] = dot(at[...], dg[j]).astype(BF16)
            mine[slot, d : 2 * d, :] = dot(at[...], du[j]).astype(BF16)
            mine[slot, 2 * d :, :] = dot(dyt[...], prod[...]).T.astype(BF16)
            tick(number * period + j, 1)
            return 0

        lax.fori_loop(0, blocks, block, 0)

        def between(v, _):
            for odd in range(2):
                leave(l, 2 * v + odd)
                enter(l - 1, 2 * v + odd)
                tick(number * period + blocks + v, odd)
            return 0

        if l > 0:
            lax.fori_loop(0, tiles // 2, between, 0)

    def drain(b, _):
        tick(b, 0)
        tick(b, 1)
        return 0

    done = (layers - 1) * period + blocks
    lax.fori_loop(done, done + (GATHER_AT[-1] + 1) // 2, drain, 0)
    for c in range(chunks):
        out_copy(c).wait()


def summed_gradients(n, x, dy, wg, wu, wd):
    layers, d, ff = wg.shape
    tokens = x.shape[1]
    blocks = ff // BLOCK
    chunks = layers * blocks
    side = math.isqrt(n)
    chunk_rows = 2 * d + BLOCK
    klass = chunk_rows // 2 // side
    piece = klass // side
    hbm = pl.BlockSpec(memory_space=pl.ANY)
    dma = pltpu.SemaphoreType.DMA
    return pl.pallas_call(
        functools.partial(train_kernel, n),
        out_shape=jax.ShapeDtypeStruct((chunks, chunk_rows, d), BF16),
        in_specs=[hbm] * 5,
        out_specs=hbm,
        scratch_shapes=[
            pltpu.VMEM((layers, tokens, d), BF16),
            pltpu.VMEM((tokens, d), BF16),
            pltpu.VMEM((tokens, d), BF16),
            pltpu.VMEM((d, tokens), BF16),
            pltpu.VMEM((d, tokens), BF16),
            pltpu.VMEM((tokens, BLOCK), BF16),
            pltpu.VMEM((blocks, tokens, BLOCK), BF16),
            pltpu.VMEM((blocks, tokens, BLOCK), BF16),
            pltpu.VMEM(((layers - 1) * blocks, chunk_rows, d), BF16),
            pltpu.VMEM((2, chunk_rows, d), BF16),
            pltpu.VMEM((2, 2, 2, klass, d // 2), BF16),
            pltpu.VMEM((2, 2, 2, klass, d), BF16),
            pltpu.VMEM((2, 2, 2, piece, d // 2), BF16),
            pltpu.VMEM((2, 2, 2, piece, d), BF16),
            pltpu.VMEM((2, 2, klass, d), F32),
            pltpu.VMEM((2, 2, 3, piece, d), BF16),
            pltpu.VMEM((chunks, chunk_rows, d), BF16),
            dma((2,)),
            dma((3, layers, blocks)),
            dma((2, 2, ROUNDS, 2)),
            dma((2, 2, ROUNDS, 2)),
            dma((chunks, 2, ROUNDS, 2)),
            dma((chunks, 2, ROUNDS, 2)),
            dma((chunks,)),
        ],
        compiler_params=pltpu.CompilerParams(collective_id=0, has_side_effects=True, vmem_limit_bytes=67043328),
        name="train",
    )(x, dy, wg, wu, wd)


def adamw_kernel(g, *refs):
    ins, outs = refs[:9], refs[9:]
    for i in range(3):
        w, m, v = (ins[i + 3 * k] for k in range(3))
        gv = g[0, i].astype(F32)
        mv = 0.9 * m[0] + 0.1 * gv
        vv = 0.95 * v[0] + 0.05 * gv * gv
        wv = w[0].astype(F32)
        step = mv * lax.rsqrt(vv + 1e-8) + 0.1 * wv
        outs[i][0] = (wv - 0.02 * step).astype(BF16)
        outs[i + 3][0] = mv
        outs[i + 6][0] = vv


def adamw(g, arrays):
    layers, d, ff = arrays[0].shape
    blocks = ff // BLOCK
    cut = 1
    size = d // cut
    g = g.reshape(layers * blocks, 3, d, BLOCK)
    wide = pl.BlockSpec((1, size, BLOCK), lambda c, r: (layers - 1 - c // blocks, r, c % blocks))
    tall = pl.BlockSpec((1, size, d), lambda c, r: (layers - 1 - c // blocks, (c % blocks) * cut + r, 0))
    specs = [wide, wide, tall] * 3
    return pl.pallas_call(
        adamw_kernel,
        grid=(layers * blocks, cut),
        out_shape=[jax.ShapeDtypeStruct(v.shape, v.dtype) for v in arrays],
        in_specs=[pl.BlockSpec((1, 3, size, BLOCK), lambda c, r: (c, 0, r, 0)), *specs],
        out_specs=specs,
        compiler_params=pltpu.CompilerParams(vmem_limit_bytes=60 * 2**20),
        name="adamw",
    )(g, *arrays)


def solution(mesh):
    n = mesh.shape["dp"]

    def step(x, dy, *arrays):
        g = summed_gradients(n, x, dy, *arrays[:3])
        return tuple(adamw(g, arrays))

    return jax.shard_map(
        step,
        mesh=mesh,
        in_specs=(P(("rep", "dp"), None, None),) * 2 + (P(None, None, None),) * 9,
        out_specs=(P("rep", None, None),) * 9,
        check_vma=False,
    )
```

```python
import functools
import math

import jax
import jax.numpy as jnp
from jax import lax
from jax.experimental import pallas as pl
from jax.experimental.pallas import tpu as pltpu
from jax.sharding import PartitionSpec as P

F32 = jnp.float32
BF16 = jnp.bfloat16
BLOCK = 512
TILE = 512
ROUNDS = 4
AHEAD = 16
SCATTER_AT = (0, 1, 3, 5, 7)
GATHER_AT = (7, 8, 10, 13, 17)


def dot(a, b):
    return jnp.dot(a, b, preferred_element_type=F32)


def dot_nt(a, b):
    return lax.dot_general(a, b, (((1,), (1,)), ((), ())), preferred_element_type=F32)


def sigmoid(x):
    return 0.5 * jnp.tanh(0.5 * x) + 0.5


def normed(wide):
    return wide * lax.rsqrt(jnp.mean(wide * wide, -1, keepdims=True) + 1e-6)


def train_kernel(n, x_hbm, dy_hbm, wg_hbm, wu_hbm, wd_hbm, out_hbm,
                 h, dy, a, at, dyt, prod, dg, du, weights,
                 mine, got_a, got_b, got_c, got_d, part, stage, whole,
                 in_sem, w_sem, rs_send, rs_recv, ag_send, ag_recv, out_sem):
    layers, d, ff = wg_hbm.shape
    tokens = x_hbm.shape[1]
    blocks = ff // BLOCK
    chunks = layers * blocks
    tiles = tokens // TILE
    period = blocks + tiles // 2
    side = math.isqrt(n)
    chunk_rows = mine.shape[1]
    half = chunk_rows // 2
    klass = half // side
    piece = klass // side
    cols = mine.shape[2]
    hc = cols // 2

    me = lax.axis_index("dp")
    cx, cy = me // side, me % side

    def near(c, by):
        return (c + by + side) % side

    ids = {
        "x": (near(cx, 1) * side + cy, near(cx, -1) * side + cy),
        "y": (cx * side + near(cy, 1), cx * side + near(cy, -1)),
    }
    sides = ((0, cx, cy, ids["x"], ids["y"]), (1, cy, cx, ids["y"], ids["x"]))

    def rows(base, size):
        return pl.ds(pl.multiple_of(base, 16), size)

    left, right = pl.ds(0, hc), pl.ds(hc, hc)
    lanes = (left, right)

    w_rows = (pl.ds(0, d), pl.ds(d, d), pl.ds(2 * d, BLOCK))

    def w_place(l, j):
        return (whole, chunks - blocks + j) if l == layers - 1 else (weights, l * blocks + j)

    def w_read(l, j, k):
        ref, i = w_place(l, j)
        return ref[i, w_rows[k], :]

    x_copy = pltpu.make_async_copy(x_hbm.at[0], h.at[0], in_sem.at[0])
    dy_copy = pltpu.make_async_copy(dy_hbm.at[0], dy, in_sem.at[1])

    def w_copies(l, j):
        span = pl.ds(j * BLOCK, BLOCK)
        ref, i = w_place(l, j)
        sources = (wg_hbm.at[l, :, span], wu_hbm.at[l, :, span], wd_hbm.at[l, span, :])
        return [pltpu.make_async_copy(src, ref.at[i, w_rows[k], :], w_sem.at[k, l, j]) for k, src in enumerate(sources)]

    x_copy.start()
    for l in range(layers):
        for j in range(blocks):
            for copy in w_copies(l, j):
                copy.start()
        if l == 0:
            dy_copy.start()

    barrier = pltpu.get_barrier_semaphore()
    for other in (*ids["x"], *ids["y"]):
        pl.semaphore_signal(barrier, inc=1, device_id={"dp": other}, device_id_type=pl.DeviceIdType.MESH)
    pl.semaphore_wait(barrier, 4)

    def rs_copy(c, hf, rnd, way, src, dst, to):
        slot = c % 2
        return pltpu.make_async_remote_copy(
            src_ref=src, dst_ref=dst, send_sem=rs_send.at[slot, hf, rnd, way], recv_sem=rs_recv.at[slot, hf, rnd, way],
            device_id={"dp": to}, device_id_type=pl.DeviceIdType.MESH)

    def rs_round(c, rnd):
        slot = c % 2
        copies = []
        for hf, f, s, fid, sid in sides:
            base = hf * half
            for way, by in ((0, 1), (1, -1)):
                if rnd == 0:
                    src = mine.at[slot, rows(base + near(f, 2) * klass, klass), lanes[way]]
                    dst, to = got_a.at[slot, hf, way], fid[way]
                elif rnd == 1:
                    src = mine.at[slot, rows(base + near(f, by) * klass, klass), :]
                    dst, to = got_b.at[slot, hf, way], fid[way]
                elif rnd == 2:
                    src = stage.at[slot, hf, 2, :, lanes[way]]
                    dst, to = got_c.at[slot, hf, way], sid[way]
                else:
                    src = stage.at[slot, hf, way]
                    dst, to = got_d.at[slot, hf, way], sid[way]
                copies.append(rs_copy(c, hf, rnd, way, src, dst, to))
        return copies

    def rs_event(c, e):
        slot = c % 2
        if e > 0:
            for copy in rs_round(c, e - 1):
                copy.wait()
        for hf, f, s, fid, sid in sides:
            base = hf * half
            if e == 1:
                for way, by in ((0, 1), (1, -1)):
                    span = rows(base + near(f, by) * klass, klass)
                    total = mine[slot, span, lanes[way]].astype(F32) + got_a[slot, hf, way].astype(F32)
                    mine[slot, span, lanes[way]] = total.astype(BF16)
            elif e == 2:
                total = mine[slot, rows(base + f * klass, klass), :].astype(F32)
                part[slot, hf] = total + got_b[slot, hf, 0].astype(F32) + got_b[slot, hf, 1].astype(F32)
                stage[slot, hf, 2] = part[slot, hf, rows(near(s, 2) * piece, piece), :].astype(BF16)
            elif e == 3:
                for way, by in ((0, 1), (1, -1)):
                    span = rows(near(s, by) * piece, piece)
                    total = part[slot, hf, span, lanes[way]] + got_c[slot, hf, way].astype(F32)
                    stage[slot, hf, way, :, lanes[way]] = total.astype(BF16)
                    stage[slot, hf, way, :, lanes[1 - way]] = part[slot, hf, span, lanes[1 - way]].astype(BF16)
            elif e == 4:
                total = part[slot, hf, rows(s * piece, piece), :]
                total = total + got_d[slot, hf, 0].astype(F32) + got_d[slot, hf, 1].astype(F32)
                whole[c, rows(base + f * klass + s * piece, piece), :] = total.astype(BF16)
        if e < ROUNDS:
            for copy in rs_round(c, e):
                copy.start()

    def ag_round(c, rnd):
        copies = []
        for hf, f, s, fid, sid in sides:
            base = hf * half
            for way, by in ((0, 1), (1, -1)):
                if rnd == 0:
                    ref = whole.at[c, rows(base + f * klass + s * piece, piece), :]
                elif rnd == 1:
                    ref = whole.at[c, rows(base + f * klass + near(s, -by) * piece, piece), lanes[way]]
                elif rnd == 2:
                    ref = whole.at[c, rows(base + f * klass, klass), :]
                else:
                    ref = whole.at[c, rows(base + near(f, -by) * klass, klass), lanes[way]]
                to = sid[way] if rnd < 2 else fid[way]
                copies.append(pltpu.make_async_remote_copy(
                    src_ref=ref, dst_ref=ref, send_sem=ag_send.at[c, hf, rnd, way], recv_sem=ag_recv.at[c, hf, rnd, way],
                    device_id={"dp": to}, device_id_type=pl.DeviceIdType.MESH))
        return copies

    def out_copy(c):
        return pltpu.make_async_copy(whole.at[c], out_hbm.at[c], out_sem.at[c])

    def ag_event(c, e):
        if e > 0:
            for copy in ag_round(c, e - 1):
                copy.wait()
        if e < ROUNDS:
            for copy in ag_round(c, e):
                copy.start()
        else:
            out_copy(c).start()

    def tick(b, odd):
        due = [(at, 0, e) for e, at in enumerate(SCATTER_AT)] + [(at, 1, e) for e, at in enumerate(GATHER_AT)]
        for at, gather, e in sorted(due, key=lambda one: (-((one[0] + 1) // 2), one[1], one[2])):
            if (at + 1) % 2 == odd:
                back = b - (at + 1) // 2 + period * AHEAD
                number, j = lax.div(back, period) - AHEAD, lax.rem(back, period)
                event = functools.partial(ag_event if gather else rs_event, number * blocks + j, e)
                pl.when((number >= 0) & (number < layers) & (j < blocks))(event)

    def enter(l, t):
        span = rows(t * TILE, TILE)
        across = pl.ds(pl.multiple_of(t * TILE, 128), TILE)
        av = normed(h[l, span, :].astype(F32)).astype(BF16)
        a[span, :] = av
        at[:, across] = av.T
        dyt[:, across] = dy[span, :].T

    x_copy.wait()
    for l in range(layers - 1):
        def arrived(l, j):
            for copy in w_copies(l, j):
                copy.wait()

        def forward(t, _):
            span = rows(t * TILE, TILE)
            wide = h[l, span, :].astype(F32)
            av = normed(wide).astype(BF16)
            acc = None
            for j in range(blocks):
                pl.when(t == 0)(functools.partial(arrived, l, j))
                gate, up = dot(av, w_read(l, j, 0)), dot(av, w_read(l, j, 1))
                p = (gate * sigmoid(gate) * up).astype(BF16)
                term = dot(p, w_read(l, j, 2))
                acc = term if acc is None else acc + term
            h[l + 1, span, :] = (wide + acc.astype(BF16).astype(F32)).astype(BF16)
            if l == layers - 2:
                pl.when(t == 0)(dy_copy.wait)
                enter(l + 1, t)
            return 0

        lax.fori_loop(0, tiles, forward, 0)

    for j in range(blocks):
        for copy in w_copies(layers - 1, j):
            copy.wait()

    def leave(l, t):
        span = rows(t * TILE, TILE)

        def back(grads, k):
            total = None
            for j in range(blocks):
                term = dot_nt(grads[j, span, :], w_read(l, j, k))
                total = term if total is None else total + term
            return total.astype(BF16).astype(F32)

        da = (back(dg, 0) + back(du, 1)).astype(BF16).astype(F32)
        wide = h[l, span, :].astype(F32)
        scale = lax.rsqrt(jnp.mean(wide * wide, -1, keepdims=True) + 1e-6)
        by_scale = jnp.sum(da * wide, -1, keepdims=True)
        by_wide = da * scale - wide * (by_scale * scale * scale * scale * (1.0 / d))
        dy[span, :] = (dy[span, :].astype(F32) + by_wide.astype(BF16).astype(F32)).astype(BF16)

    for number, l in enumerate(reversed(range(layers))):

        def block(j, _):
            c = number * blocks + j
            slot = c % 2

            def tile(t, _):
                span = rows(t * TILE, TILE)
                av, dyv = a[span, :], dy[span, :]
                gate, up = dot(av, w_read(l, j, 0)), dot(av, w_read(l, j, 1))
                dp = dot_nt(dyv, w_read(l, j, 2)).astype(BF16).astype(F32)
                sig = sigmoid(gate)
                act = gate * sig
                prod[span, :] = (act * up).astype(BF16)
                dgv = (dp * up * (sig + act * (1.0 - sig))).astype(BF16)
                duv = (dp * act).astype(BF16)
                dg[j, span, :] = dgv
                du[j, span, :] = duv
                return 0

            lax.fori_loop(0, tiles, tile, 0)
            tick(number * period + j, 0)
            mine[slot, 0:d, :] = dot(at[...], dg[j]).astype(BF16)
            mine[slot, d : 2 * d, :] = dot(at[...], du[j]).astype(BF16)
            mine[slot, 2 * d :, :] = dot(dyt[...], prod[...]).T.astype(BF16)
            tick(number * period + j, 1)
            return 0

        lax.fori_loop(0, blocks, block, 0)

        def between(v, _):
            for odd in range(2):
                leave(l, 2 * v + odd)
                enter(l - 1, 2 * v + odd)
                tick(number * period + blocks + v, odd)
            return 0

        if l > 0:
            lax.fori_loop(0, tiles // 2, between, 0)

    def drain(b, _):
        tick(b, 0)
        tick(b, 1)
        return 0

    done = (layers - 1) * period + blocks
    lax.fori_loop(done, done + (GATHER_AT[-1] + 1) // 2, drain, 0)
    for c in range(chunks):
        out_copy(c).wait()


def summed_gradients(n, x, dy, wg, wu, wd):
    layers, d, ff = wg.shape
    tokens = x.shape[1]
    blocks = ff // BLOCK
    chunks = layers * blocks
    side = math.isqrt(n)
    chunk_rows = 2 * d + BLOCK
    klass = chunk_rows // 2 // side
    piece = klass // side
    hbm = pl.BlockSpec(memory_space=pl.ANY)
    dma = pltpu.SemaphoreType.DMA
    return pl.pallas_call(
        functools.partial(train_kernel, n),
        out_shape=jax.ShapeDtypeStruct((chunks, chunk_rows, d), BF16),
        in_specs=[hbm] * 5,
        out_specs=hbm,
        scratch_shapes=[
            pltpu.VMEM((layers, tokens, d), BF16),
            pltpu.VMEM((tokens, d), BF16),
            pltpu.VMEM((tokens, d), BF16),
            pltpu.VMEM((d, tokens), BF16),
            pltpu.VMEM((d, tokens), BF16),
            pltpu.VMEM((tokens, BLOCK), BF16),
            pltpu.VMEM((blocks, tokens, BLOCK), BF16),
            pltpu.VMEM((blocks, tokens, BLOCK), BF16),
            pltpu.VMEM(((layers - 1) * blocks, chunk_rows, d), BF16),
            pltpu.VMEM((2, chunk_rows, d), BF16),
            pltpu.VMEM((2, 2, 2, klass, d // 2), BF16),
            pltpu.VMEM((2, 2, 2, klass, d), BF16),
            pltpu.VMEM((2, 2, 2, piece, d // 2), BF16),
            pltpu.VMEM((2, 2, 2, piece, d), BF16),
            pltpu.VMEM((2, 2, klass, d), F32),
            pltpu.VMEM((2, 2, 3, piece, d), BF16),
            pltpu.VMEM((chunks, chunk_rows, d), BF16),
            dma((2,)),
            dma((3, layers, blocks)),
            dma((2, 2, ROUNDS, 2)),
            dma((2, 2, ROUNDS, 2)),
            dma((chunks, 2, ROUNDS, 2)),
            dma((chunks, 2, ROUNDS, 2)),
            dma((chunks,)),
        ],
        compiler_params=pltpu.CompilerParams(collective_id=0, has_side_effects=True, vmem_limit_bytes=67043328),
        name="train",
    )(x, dy, wg, wu, wd)


def adamw_kernel(g, *refs):
    ins, outs = refs[:9], refs[9:]
    for i in range(3):
        w, m, v = (ins[i + 3 * k] for k in range(3))
        gv = g[0, i].astype(F32)
        mv = 0.9 * m[0] + 0.1 * gv
        vv = 0.95 * v[0] + 0.05 * gv * gv
        wv = w[0].astype(F32)
        step = mv * lax.rsqrt(vv + 1e-8) + 0.1 * wv
        outs[i][0] = (wv - 0.02 * step).astype(BF16)
        outs[i + 3][0] = mv
        outs[i + 6][0] = vv


def adamw(g, arrays):
    layers, d, ff = arrays[0].shape
    blocks = ff // BLOCK
    cut = 1
    size = d // cut
    g = g.reshape(layers * blocks, 3, d, BLOCK)
    wide = pl.BlockSpec((1, size, BLOCK), lambda c, r: (layers - 1 - c // blocks, r, c % blocks))
    tall = pl.BlockSpec((1, size, d), lambda c, r: (layers - 1 - c // blocks, (c % blocks) * cut + r, 0))
    specs = [wide, wide, tall] * 3
    return pl.pallas_call(
        adamw_kernel,
        grid=(layers * blocks, cut),
        out_shape=[jax.ShapeDtypeStruct(v.shape, v.dtype) for v in arrays],
        in_specs=[pl.BlockSpec((1, 3, size, BLOCK), lambda c, r: (c, 0, r, 0)), *specs],
        out_specs=specs,
        compiler_params=pltpu.CompilerParams(vmem_limit_bytes=60 * 2**20),
        name="adamw",
    )(g, *arrays)


def solution(mesh):
    n = mesh.shape["dp"]

    def step(x, dy, *arrays):
        g = summed_gradients(n, x, dy, *arrays[:3])
        return tuple(adamw(g, arrays))

    return jax.shard_map(
        step,
        mesh=mesh,
        in_specs=(P(("rep", "dp"), None, None),) * 2 + (P(None, None, None),) * 9,
        out_specs=(P("rep", None, None),) * 9,
        check_vma=False,
    )
```
